256 devices in a mesh: field: 4 (over y, x), ep: 64 (over z, core).
Axes of the slice: x: 2, y: 2, z: 32, core: 2. Of those that a mesh axis runs over, the one named last changes fastest.
The devices are a block of a 4x8x32 slice.
Arguments:
- images: float32 [512, 64, 256], P(('field', 'ep')), parts along dimension 0, may hold values from -6 to 6
- reference_image: float32 [256, 256], P('field'), parts along dimension 0, may hold values from -6 to 6
- kernels: float32 [16, 23, 23], replicated, may hold values from -0.25 to 0.25
- kernel_index: int32 [512], P(('field', 'ep')), parts along dimension 0, may hold values from 0 to 15
- tile_mask: int32 [512, 64, 2], P(('field', 'ep')), parts along dimension 0, may hold values 0 or 1
- systematics: float32 [512, 40], P('field'), parts along dimension 0, may hold values from -6 to 6
- onsets: int32 [32], P('field'), parts along dimension 0, may hold values from 0 to 123
Outputs:
- coefficients: float32 [48, 256, 256], P(None, ('field', 'ep')), parts along dimension 1
- epoch_scatter: float32 [512], P('field'), parts along dimension 0
The draws below stay inside these ranges and needn't reach their ends.
There are 4 independent parts, one for each index of `field`. The reference program is written for one: setup_inputs(seed, part) draws one part's arguments, and reference() takes and returns one part's arrays. A program takes and returns all parts, laid end to end along the dimension named above; an argument that names none is the same for every part. Nothing has to cross between parts.
All inputs are finite; a program needn't handle non-finite values. No bound on the sum of `tile_mask` on one device may be relied on, other than what follows from the above.
Results may differ from the reference program's by a relative error of at most 0.00011.
Values sent between devices are 32-bit elements; how exact they have to be, the bound alone decides.
A program may use at most 64 MiB of HBM per device.

```python
import jax
import jax.numpy as jnp
from jax import lax

W = 256
KS = 23
NK = 16
NSYS = 40
NTR = 8
R = 64
E = 128


def touch_ends(drawn, stream_key, smallest, high):
    dims = drawn.shape
    spot = [jax.random.randint(jax.random.fold_in(stream_key, axis), (), 0, dims[axis]) for axis in range(len(dims))]
    drawn = drawn.at[tuple(spot)].set(smallest)
    longest = dims.index(max(dims))
    spot[longest] = (spot[longest] + 1) % dims[longest]
    return drawn.at[tuple(spot)].set(high)


def block_levels(rng, dims, cuts, least, largest):
    level, own = 1.0, jax.random.fold_in(rng, 6)
    for position, shards_of in cuts:
        steps = jnp.exp(jax.random.uniform(jax.random.fold_in(own, position), (shards_of,), jnp.float32, least / len(cuts), largest / len(cuts)))
        level = level * jnp.repeat(steps, dims[position] // shards_of).reshape([-1 if axis == position else 1 for axis in range(len(dims))])
    return level


def noise(stream_key, dims, scale, reach, shards=(), kind=jnp.bfloat16):
    factor_of = block_levels(stream_key, dims, shards, -0.22, 0.18) if shards else 1.0
    values = jax.random.normal(stream_key, dims, jnp.float32) * scale * factor_of
    return jnp.minimum(jnp.maximum(values, -reach), reach).astype(kind)


def setup_inputs(seed: int = 0, part: int = 0) -> dict:
    splits = jax.random.split(jax.random.key(seed), 8)
    own_keys = jax.random.split(jax.random.fold_in(splits[7], part), 8)
    images = noise(own_keys[0], (E, R, W), 1.0, 6.0, ((0, 64),), jnp.float32)
    reference_image = noise(own_keys[1], (R, W), 1.0, 6.0, (), jnp.float32)
    kernels = noise(splits[2], (NK, KS, KS), (KS * KS) ** -0.5, 0.25, (), jnp.float32)
    kernel_index = touch_ends(jax.random.randint(own_keys[3], (E,), 0, NK), jax.random.fold_in(own_keys[3], 1), 0, NK - 1).astype(jnp.int32)
    tile_mask = touch_ends((jax.random.randint(own_keys[4], (E, R, W // 128), 0, 8) < 7).astype(jnp.int32), jax.random.fold_in(own_keys[4], 1), 0, 1)
    systematics = noise(own_keys[5], (E, NSYS), 1.0, 6.0, (), jnp.float32)
    onsets = touch_ends(jax.random.randint(own_keys[6], (NTR,), 0, E - 4), jax.random.fold_in(own_keys[6], 1), 0, (E - 4) - 1).astype(jnp.int32)
    return dict(images=images, reference_image=reference_image, kernels=kernels, kernel_index=kernel_index, tile_mask=tile_mask, systematics=systematics, onsets=onsets)


cov_ridge = 0.5
fit_ridge = 1.0

def correlate(stack, chosen):
    count = stack.shape[0]
    filters = jnp.transpose(chosen, (1, 2, 0))[:, :, None, :]
    result = lax.conv_general_dilated(stack[None], filters, (1, 1), 'SAME', dimension_numbers=('NCHW', 'HWIO', 'NCHW'), feature_group_count=count, precision=lax.Precision.HIGHEST)
    return result[0]

def subtract(stack, reference_image, chosen, masks):
    result = reference_image[None] - correlate(stack, chosen)
    shape = result.shape
    tiles = result.reshape(shape[0], shape[1], shape[2] // 128, 128) * masks[..., None].astype(jnp.float32)
    return tiles.reshape(shape)

def build_design(systematics, onsets):
    count = systematics.shape[0]
    templates = onsets.shape[0]
    epoch_axis = jnp.arange(count, dtype=jnp.float32)[:, None]
    delays = epoch_axis - onsets[None, :].astype(jnp.float32)
    timescale = (jnp.arange(templates, dtype=jnp.float32) + 1.0) * count / (2.0 * templates)
    transient = jnp.where(delays >= 0.0, jnp.exp(-jnp.maximum(delays, 0.0) / timescale[None, :]), 0.0)
    return jnp.concatenate([systematics, transient.astype(systematics.dtype)], axis=1)

def fit_matrix(scatter, npixels, design):
    count = design.shape[0]
    columns = design.shape[1]
    covariance = scatter / npixels + cov_ridge * jnp.eye(count, dtype=scatter.dtype)
    lower = jnp.linalg.cholesky(covariance)
    weighted = jax.scipy.linalg.cho_solve((lower, True), design)
    normal = jnp.dot(design.T, weighted, precision=lax.Precision.HIGHEST) + fit_ridge * jnp.eye(columns, dtype=scatter.dtype)
    lower_fit = jnp.linalg.cholesky(normal)
    return jax.scipy.linalg.cho_solve((lower_fit, True), weighted.T)

def reference(images, reference_image, kernels, kernel_index, tile_mask, systematics, onsets):
    count, rows, width = images.shape
    chosen = kernels[kernel_index]
    difference = subtract(images, reference_image, chosen, tile_mask)
    pixel_data = difference.reshape(count, rows * width)
    scatter = jnp.dot(pixel_data, pixel_data.T, precision=lax.Precision.HIGHEST)
    npixels = float(rows * width)
    design = build_design(systematics, onsets)
    fit = fit_matrix(scatter, npixels, design)
    coefficients = jnp.dot(fit, pixel_data, precision=lax.Precision.HIGHEST)
    residual = pixel_data - jnp.dot(design, coefficients, precision=lax.Precision.HIGHEST)
    epoch_scatter = jnp.sum(residual * residual, axis=1) / npixels
    return (coefficients.reshape(design.shape[1], rows, width), epoch_scatter)
```

```python
import functools

import jax
import jax.numpy as jnp
from jax import lax
from jax.experimental import pallas as pl
from jax.experimental.pallas import tpu as pltpu
from jax.sharding import PartitionSpec as P

f32, bf16, i32 = jnp.float32, jnp.bfloat16, jnp.int32
HIGHEST = lax.Precision.HIGHEST
cov_ridge = 0.5
LANES = 128


def split(x):
    high = x.astype(bf16).astype(f32)
    return high, x - high


def iota(shape, axis):
    return lax.broadcasted_iota(i32, shape, axis)


def correlate(image, kernel, kpad, bands, shifted):
    side = kernel.shape[0]
    half = side // 2
    rows = image.shape[0]
    kpad[...] = jnp.zeros_like(kpad)
    kpad[0:side, 0:side] = kernel
    high, low = split(kpad[...].T)
    base = pltpu.roll(high, LANES - half, 1) + pltpu.roll(low, rows - half, 1)
    lane = iota((rows, LANES), 1)
    band = jnp.abs(lax.rem(lane, rows) - iota((rows, LANES), 0)) <= half
    for b in range(side):
        column = jnp.broadcast_to(base[b : b + 1, :], (rows, LANES))
        column = pltpu.roll(column, 0, 1, stride=1, stride_axis=0)
        bands[b * rows : (b + 1) * rows, :] = jnp.where(band, column, 0.0).astype(bf16)
    high, low = split(image)
    high, low = high.astype(bf16), low.astype(bf16)
    left = bands[...]
    shifted[...] = jnp.dot(
        jnp.concatenate([left, left], axis=1),
        jnp.concatenate([high, high, low, low], axis=0),
        preferred_element_type=f32,
    )
    total = [None, None]
    for b in range(side):
        s = b - half
        block = slice(b * rows, (b + 1) * rows)
        first, second = shifted[block, 0:LANES], shifted[block, LANES:]
        if s:
            x = pltpu.roll(first, (-s) % LANES, 1)
            y = pltpu.roll(second, (-s) % LANES, 1)
            if s > 0:
                inside = lane < LANES - s
                first, second = jnp.where(inside, x, y), jnp.where(inside, y, 0.0)
            else:
                inside = lane >= -s
                first, second = jnp.where(inside, x, 0.0), jnp.where(inside, y, x)
        total = [v if t is None else t + v for t, v in zip(total, (first, second))]
    return total


def eliminate(matrix, right):
    count = matrix.shape[0]
    width = 8
    row8 = iota((width, LANES), 0)
    for k in range(0, count, width):
        pivot = slice(k, k + width)
        columns = [
            jnp.broadcast_to(matrix[:, k + j : k + j + 1], (count, LANES)) for j in range(width)
        ]
        block = [c[pivot, :] for c in columns]
        a, x = matrix[pivot, :], right[pivot, :]
        for j in range(width):
            factor = block[j]
            inverse = 1.0 / factor[j : j + 1, :]

            def step(v):
                scaled = v[j : j + 1, :] * inverse
                return jnp.where(row8 == j, scaled, v - factor * scaled)

            a, x = step(a), step(x)
            for m in range(j + 1, width):
                block[m] = step(block[m])

        def update(value, rows):
            for j in range(width):
                value = value - columns[j] * rows[j : j + 1, :]
            above = [value[:k, :]] if k else []
            below = [value[k + width :, :]] if k + width < count else []
            return jnp.concatenate([*above, rows, *below], axis=0)

        if k + width < count:
            matrix = update(matrix, a)
        right = update(right, x)
    return right


def body(
    devices,
    index_ref,
    onsets_ref,
    images_ref,
    reference_ref,
    kernels_ref,
    mask_ref,
    systematics_ref,
    coefficients_ref,
    scatter_ref,
    kpad,
    bands,
    shifted,
    parcel,
    inbox,
    pair_box,
    half_sum,
    gathered,
    fit_ref,
    spare,
    residual_ref,
    design_ref,
    sems,
    fit_send,
    fit_got,
    residual_send,
    residual_got,
):
    local, rows, width = images_ref.shape
    owners = devices // 2
    me = lax.axis_index("ep")
    core = lax.rem(me, 2)
    partner = me + 1 - 2 * core
    root = 1
    epochs = systematics_ref.shape[0]
    pixels = float(rows * width)

    def remote(source, target, sems, device):
        send, receive = sems
        return pltpu.make_async_remote_copy(
            src_ref=source,
            dst_ref=target,
            send_sem=send,
            recv_sem=receive,
            device_id={"ep": device},
        )

    parcel_sems, pair_sems, gather_sems, row_sems = (
        (sems.at[2 * i], sems.at[2 * i + 1]) for i in range(4)
    )

    is_owner = me < owners
    barrier = pltpu.get_barrier_semaphore()

    @pl.when(is_owner)
    def _():
        @pl.loop(1, devices)
        def _(step):
            pl.semaphore_signal(barrier, inc=1, device_id={"ep": lax.rem(me + step, devices)})

    for e in range(local):
        conv = correlate(
            images_ref[e], kernels_ref[:, index_ref[e], :], kpad.at[e], bands.at[e], shifted.at[e]
        )
        for t in range(width // LANES):
            lanes = slice(t * LANES, (t + 1) * LANES)
            good = jnp.broadcast_to(mask_ref[e, :, t : t + 1].astype(f32), (rows, LANES))
            difference = (reference_ref[:, lanes] - conv[t]) * good
            for k in range(2):
                parcel[pl.ds(k * 4 + t * 2 + e, owners, stride=8), :] = difference[
                    k * owners : (k + 1) * owners, :
                ]

    @pl.when(is_owner)
    def _():
        pl.semaphore_wait(barrier, owners - 1)

    @pl.when(jnp.logical_not(is_owner))
    def _():
        pl.semaphore_wait(barrier, owners)

    def tile(ref, index):
        return ref.at[pl.ds(pl.multiple_of(index * 8, 8), 8), :]

    def send_to(owner):
        @pl.when(owner != me)
        def _():
            remote(tile(parcel, owner), tile(inbox, me), parcel_sems, owner).start()

    @pl.loop(0, owners)
    def _(step):
        send_to(owners - 1 - step)

    @pl.when(is_owner)
    def _():
        inbox[pl.ds(pl.multiple_of(me * 8, 8), 8), :] = parcel[
            pl.ds(pl.multiple_of(me * 8, 8), 8), :
        ]
        arrived = inbox.at[pl.ds(0, (devices - 1) * 8), :]
        remote(arrived, arrived, parcel_sems, partner).wait_recv()
        sent = parcel.at[pl.ds(0, (owners - 1) * 8), :]
        remote(sent, sent, parcel_sems, partner).wait_send()

    @pl.when(jnp.logical_not(is_owner))
    def _():
        remote(parcel, parcel, parcel_sems, partner).wait_send()

    def order(ref_rows):
        return [ref_rows(h, e) for h in range(2) for e in range(local)]

    def data(k, t):
        return jnp.concatenate(
            order(
                lambda h, e: inbox[
                    pl.ds(h * owners * 8 + k * 4 + t * 2 + e, owners, stride=8), :
                ]
            ),
            axis=0,
        )

    nt = (((1,), (1,)), ((), ()))

    def dot_nt(x, y):
        return lax.dot_general(x, y, nt, precision=HIGHEST, preferred_element_type=f32)

    fit_rows = fit_ref.shape[0]
    half = epochs // 2

    @pl.when(is_owner)
    def _():
        pieces = [data(k, t) for k in range(2) for t in range(2)]
        total = sum(dot_nt(d, d) for d in pieces)
        half_sum[...] = total

        def part(which):
            return half_sum.at[pl.ds(pl.multiple_of(which * half, half), half), :]

        pair = remote(part(1 - core), pair_box, pair_sems, partner)
        pair.start()
        pair.wait_recv()
        mine = half_sum[pl.ds(pl.multiple_of(core * half, half), half), :] + pair_box[...]
        slot = gathered.at[me]

        @pl.when(me == root)
        def _():
            gathered[me] = mine

        @pl.when(me != root)
        def _():
            spare[...] = mine
            copy = remote(spare, slot, gather_sems, root)
            copy.start()
            copy.wait_send()

        pair.wait_send()

    @pl.when(me == root)
    def _():
        design_ref[...] = jnp.zeros_like(design_ref)
        known = systematics_ref.shape[1]
        for h in range(2):
            for e in range(local):
                at = (h * local + e) * owners
                design_ref[at : at + owners, 0:known] = systematics_ref[
                    pl.ds(h * owners * local + e, owners, stride=local), :
                ]
        templates = onsets_ref.shape[0]
        lane = iota((epochs, LANES), 1)
        place = iota((epochs, LANES), 0)
        position = lax.rem(place, owners)
        group = place // owners
        epoch = (position + (group // local) * owners) * local + lax.rem(group, local)
        onset = jnp.zeros((epochs, LANES), f32)
        for k in range(templates):
            onset = jnp.where(lane == known + k, onsets_ref[k].astype(f32), onset)
        delay = epoch.astype(f32) - onset
        timescale = (lane - known + 1).astype(f32) * epochs / (2.0 * templates)
        is_template = jnp.logical_and(lane >= known, lane < known + templates)
        timescale = jnp.where(is_template, timescale, 1.0)
        transient = jnp.where(delay >= 0.0, jnp.exp(-jnp.maximum(delay, 0.0) / timescale), 0.0)
        design = jnp.where(is_template, transient, design_ref[...])
        base = dot_nt(design, design)
        diagonal = iota((epochs, LANES), 0) == lane
        base = base + jnp.where(diagonal, cov_ridge, 0.0)

        slots = gathered.at[pl.ds(0, owners - 1)]
        remote(slots, slots, gather_sems, partner).wait_recv()
        total = [jnp.zeros((half, LANES), f32)] * 2
        for c in range(0, owners, 2):
            total = [t + gathered[c + s] for s, t in enumerate(total)]
        scatter = jnp.concatenate(total, axis=0)
        gain = eliminate(base + scatter / pixels, design)
        fit_ref[...] = gain.T[0:fit_rows, :]

        @pl.loop(0, owners)
        def _(step):
            @pl.when(step != me)
            def _():
                remote(fit_ref, fit_ref, (fit_send.at[step], fit_got), step).start()

        projector = jnp.where(diagonal, 1.0, 0.0) - dot_nt(design, gain)
        product = jnp.dot(projector, scatter, precision=HIGHEST, preferred_element_type=f32)
        terms = product * projector
        for h in range(2):
            for e in range(local):
                at = (h * local + e) * owners
                design_ref[pl.ds(h * owners * local + e, owners, stride=local), :] = terms[
                    at : at + owners, :
                ]
        residual = jnp.sum(design_ref[...].T, axis=0, keepdims=True) / pixels
        residual_ref[...] = jnp.broadcast_to(residual, residual_ref.shape)
        scatter_ref[...] = jnp.broadcast_to(residual, scatter_ref.shape)

        @pl.loop(1, devices)
        def _(step):
            other = lax.rem(me + step, devices)
            remote(
                residual_ref, scatter_ref, (residual_send.at[step], residual_got), other
            ).start()

    @pl.when(is_owner)
    def _():
        @pl.when(me != root)
        def _():
            remote(fit_ref, fit_ref, (fit_send.at[0], fit_got), partner).wait_recv()

        def row(k):
            fit = fit_ref[...]
            return jnp.concatenate(
                [
                    jnp.dot(fit, data(k, t), precision=HIGHEST, preferred_element_type=f32)
                    for t in range(2)
                ],
                axis=1,
            )

        coefficients_ref[...] = row(0)
        shifted[0, 0:fit_rows, :] = row(1)
        source = shifted.at[0, pl.ds(0, fit_rows), :]
        copy = remote(source, coefficients_ref, row_sems, me + owners)
        copy.start()
        copy.wait_send()

    @pl.when(jnp.logical_not(is_owner))
    def _():
        remote(coefficients_ref, coefficients_ref, row_sems, partner).wait_recv()

    @pl.when(me != root)
    def _():
        remote(
            residual_ref, scatter_ref, (residual_send.at[0], residual_got), partner
        ).wait_recv()

    @pl.when(me == root)
    def _():
        @pl.loop(0, owners)
        def _(step):
            @pl.when(step != me)
            def _():
                remote(fit_ref, fit_ref, (fit_send.at[step], fit_got), partner).wait_send()

        @pl.loop(1, devices)
        def _(step):
            remote(
                residual_ref, scatter_ref, (residual_send.at[step], residual_got), partner
            ).wait_send()


def shards(
    devices, images, reference_image, kernels, kernel_index, tile_mask, systematics, onsets
):
    local, rows, width = images.shape
    side = kernels.shape[1]
    epochs = systematics.shape[0]
    columns = systematics.shape[1] + onsets.shape[0]
    owners = devices // 2
    vmem = pl.BlockSpec(memory_space=pltpu.VMEM)
    smem = pl.BlockSpec(memory_space=pltpu.SMEM)
    coefficients, scatter = pl.pallas_call(
        functools.partial(body, devices),
        out_shape=(
            jax.ShapeDtypeStruct((columns, width), f32),
            jax.ShapeDtypeStruct((8, epochs), f32),
        ),
        in_specs=[smem, smem, vmem, vmem, vmem, vmem, vmem],
        out_specs=(vmem, vmem),
        scratch_shapes=[
            pltpu.VMEM((local, LANES, LANES), f32),
            pltpu.VMEM((local, side * rows, LANES), bf16),
            pltpu.VMEM((local, side * rows, width), f32),
            pltpu.VMEM((owners * 8, LANES), f32),
            pltpu.VMEM((devices * 8, LANES), f32),
            pltpu.VMEM((epochs // 2, epochs), f32),
            pltpu.VMEM((epochs, epochs), f32),
            pltpu.VMEM((owners, epochs // 2, epochs), f32),
            pltpu.VMEM((columns, epochs), f32),
            pltpu.VMEM((epochs // 2, epochs), f32),
            pltpu.VMEM((8, epochs), f32),
            pltpu.VMEM((epochs, LANES), f32),
            pltpu.SemaphoreType.DMA((8,)),
            pltpu.SemaphoreType.DMA((owners,)),
            pltpu.SemaphoreType.DMA,
            pltpu.SemaphoreType.DMA((devices,)),
            pltpu.SemaphoreType.DMA,
        ],
        compiler_params=pltpu.CompilerParams(collective_id=0, has_side_effects=True),
    )(
        kernel_index,
        onsets,
        images,
        reference_image,
        jnp.transpose(kernels, (1, 0, 2)),
        tile_mask,
        systematics,
    )
    return coefficients[:, None, :], scatter[0]


def solution(mesh):
    in_specs = (
        P(("field", "ep"), None, None),
        P("field", None),
        P(),
        P(("field", "ep")),
        P(("field", "ep"), None, None),
        P("field", None),
        P("field"),
    )
    out_specs = (P(None, ("field", "ep"), None), P("field"))
    return jax.shard_map(
        functools.partial(shards, mesh.shape["ep"]),
        mesh=mesh,
        in_specs=in_specs,
        out_specs=out_specs,
        check_vma=False,
    )
```

```python
import functools

import jax
import jax.numpy as jnp
from jax import lax
from jax.experimental import pallas as pl
from jax.experimental.pallas import tpu as pltpu
from jax.sharding import PartitionSpec as P

f32, bf16, i32 = jnp.float32, jnp.bfloat16, jnp.int32
HIGHEST = lax.Precision.HIGHEST
cov_ridge = 0.5
LANES = 128


def split(x):
    high = x.astype(bf16).astype(f32)
    return high, x - high


def pieces(x):
    high, low = split(x)
    return high.astype(bf16), low.astype(bf16)


def iota(shape, axis):
    return lax.broadcasted_iota(i32, shape, axis)


def correlate(image, kernel, kpad, bands, shifted):
    side = kernel.shape[0]
    half = side // 2
    rows = image.shape[0]
    kpad[...] = jnp.zeros_like(kpad)
    kpad[0:side, 0:side] = kernel
    high, low = split(kpad[...].T)
    base = pltpu.roll(high, LANES - half, 1) + pltpu.roll(low, rows - half, 1)
    lane = iota((rows, LANES), 1)
    band = jnp.abs(lax.rem(lane, rows) - iota((rows, LANES), 0)) <= half
    for b in range(side):
        column = jnp.broadcast_to(base[b : b + 1, :], (rows, LANES))
        column = pltpu.roll(column, 0, 1, stride=1, stride_axis=0)
        bands[b * rows : (b + 1) * rows, :] = jnp.where(band, column, 0.0).astype(bf16)
    high, low = pieces(image)
    left = bands[...]
    shifted[...] = jnp.dot(
        jnp.concatenate([left, left], axis=1),
        jnp.concatenate([high, high, low, low], axis=0),
        preferred_element_type=f32,
    )
    total = [None, None]
    for b in range(side):
        s = b - half
        block = slice(b * rows, (b + 1) * rows)
        first, second = shifted[block, 0:LANES], shifted[block, LANES:]
        if s:
            x = pltpu.roll(first, (-s) % LANES, 1)
            y = pltpu.roll(second, (-s) % LANES, 1)
            if s > 0:
                inside = lane < LANES - s
                first, second = jnp.where(inside, x, y), jnp.where(inside, y, 0.0)
            else:
                inside = lane >= -s
                first, second = jnp.where(inside, x, 0.0), jnp.where(inside, y, x)
        total = [v if t is None else t + v for t, v in zip(total, (first, second))]
    return total


def eliminate(matrix, right):
    count = matrix.shape[0]
    width = 8
    row8 = iota((width, LANES), 0)
    for k in range(0, count, width):
        pivot = slice(k, k + width)
        columns = [
            jnp.broadcast_to(matrix[:, k + j : k + j + 1], (count, LANES)) for j in range(width)
        ]
        block = [c[pivot, :] for c in columns]
        a, x = matrix[pivot, :], right[pivot, :]
        for j in range(width):
            factor = block[j]
            inverse = 1.0 / factor[j : j + 1, :]

            def step(v):
                scaled = v[j : j + 1, :] * inverse
                return jnp.where(row8 == j, scaled, v - factor * scaled)

            a, x = step(a), step(x)
            for m in range(j + 1, width):
                block[m] = step(block[m])

        def update(value, rows):
            for j in range(width):
                value = value - columns[j] * rows[j : j + 1, :]
            above = [value[:k, :]] if k else []
            below = [value[k + width :, :]] if k + width < count else []
            return jnp.concatenate([*above, rows, *below], axis=0)

        if k + width < count:
            matrix = update(matrix, a)
        right = update(right, x)
    return right


NT = (((1,), (1,)), ((), ()))


def dot_nt(x, y):
    return lax.dot_general(x, y, NT, precision=HIGHEST, preferred_element_type=f32)


def gram(x):
    high, low = pieces(x)
    left = jnp.concatenate([high, high, low], axis=1)
    right = jnp.concatenate([high, low, high], axis=1)
    return lax.dot_general(left, right, NT, preferred_element_type=f32)


def fold(value):
    tiles = LANES // 8
    lane = iota((8, LANES), 1)
    block = [value[8 * i : 8 * i + 8, :] for i in range(tiles)]
    folded, last = [], jnp.zeros((8, LANES), f32)
    for i in range(tiles // 2):
        other = block[tiles - 1 - i]
        moved = pltpu.roll(other, 8 * i, 1) if i else other
        folded.append(jnp.where(lane >= 8 * i, block[i], moved))
        last = jnp.where(lane // 8 == tiles - 1 - i, other, last)
    return [*folded, last]


def unfold(folded):
    tiles = LANES // 8
    lane = iota((8, LANES), 1)
    above, blocks = [None] * tiles, [None] * tiles
    for i in range(tiles // 2):
        other = tiles - 1 - i
        moved = pltpu.roll(folded[i], LANES - 8 * i, 1) if i else folded[i]
        above[i] = jnp.where(lane >= 8 * i + 8, folded[i], 0.0)
        above[other] = jnp.where(lane >= 8 * other + 8, moved, 0.0)
        blocks[i] = jnp.where(lane // 8 == i, folded[i], 0.0)
        blocks[other] = jnp.where(lane // 8 == other, folded[-1], 0.0)
    above = jnp.concatenate(above, axis=0)
    return above + above.T + jnp.concatenate(blocks, axis=0)


def body(
    devices,
    index_ref,
    onsets_ref,
    images_ref,
    reference_ref,
    kernels_ref,
    mask_ref,
    systematics_ref,
    coefficients_ref,
    residual_ref,
    kpad,
    bands,
    shifted,
    parcel,
    inbox,
    relay,
    folded_ref,
    pair_box,
    sum_ref,
    gathered,
    fit_ref,
    row_ref,
    mask_pad,
    design_ref,
    sems,
    parcel_send,
    relay_send,
    relay_got,
    fit_send,
    residual_send,
):
    local, rows, width = images_ref.shape
    epochs = systematics_ref.shape[1]
    owners = devices // 2
    near = owners // 2
    root = 1
    pixels = float(rows * width)
    me = lax.axis_index("ep")
    core = lax.rem(me, 2)
    partner = me + 1 - 2 * core
    is_owner = me < owners
    is_late = jnp.logical_not(is_owner)

    def remote(source, target, send, receive, device):
        return pltpu.make_async_remote_copy(
            src_ref=source,
            dst_ref=target,
            send_sem=send,
            recv_sem=receive,
            device_id={"ep": device},
        )

    def tile(ref, index):
        return ref.at[pl.ds(pl.multiple_of(index * 8, 8), 8), :]

    def relayed(owner, late):
        return jnp.logical_and(owner >= near, owner // 2 <= late // 2 - near)

    barrier = pltpu.get_barrier_semaphore()

    @pl.when(is_owner)
    def _():
        @pl.loop(1, devices)
        def _(step):
            other = lax.rem(me + step, devices)

            @pl.when(jnp.logical_not(jnp.logical_and(other >= owners, relayed(me, other))))
            def _():
                pl.semaphore_signal(barrier, inc=1, device_id={"ep": other})

    mask_pad[...] = jnp.zeros_like(mask_pad)
    halves = width // LANES
    for e in range(local):
        mask_pad[e * halves : (e + 1) * halves, 0:rows] = mask_ref[e].astype(f32)
    mask = mask_pad[...].T

    for e in range(local):
        conv = correlate(
            images_ref[e], kernels_ref[:, index_ref[e], :], kpad.at[e], bands.at[e], shifted.at[e]
        )
        for t in range(halves):
            lanes = slice(t * LANES, (t + 1) * LANES)
            column = e * halves + t
            good = jnp.broadcast_to(mask[0:rows, column : column + 1], (rows, LANES))
            difference = (reference_ref[:, lanes] - conv[t]) * good
            parcel[pl.ds(t * 2 + e, owners, stride=8), :] = difference[:owners, :]
            parcel[pl.ds(4 + t * 2 + e, near, stride=8), :] = difference[owners + near :, :]
            parcel[pl.ds(near * 8 + 4 + t * 2 + e, near, stride=8), :] = difference[
                owners : owners + near, :
            ]

    served = owners + lax.rem(me + near, owners)
    got_parcel = sems.at[0]

    @pl.when(is_owner)
    def _():
        pl.semaphore_wait(barrier, owners - 1)

    @pl.when(is_late)
    def _():
        direct = jnp.minimum(near // 2, devices // 2 - 1 - me // 2)
        pl.semaphore_wait(barrier, near + 2 * direct)

    for owner in reversed(range(owners)):
        source = parcel.at[pl.ds(owner * 8, 8), :]
        through = jnp.logical_and(is_late, relayed(owner, me)) if owner >= near else False

        def direct(owner=owner, source=source):
            remote(source, tile(inbox, me), parcel_send, got_parcel, owner).start()

        if owner >= near:

            @pl.when(through)
            def _(owner=owner, source=source):
                place = me - (owners + near)
                target = tile(relay, place)
                remote(source, target, parcel_send, relay_got.at[place], owner - near).start()

        @pl.when(jnp.logical_and(owner != me, jnp.logical_not(through)))
        def _(direct=direct):
            direct()

    @pl.when(me < near)
    def _():
        @pl.loop(0, near)
        def _(step):
            place = near - 1 - step
            late = place + owners + near

            @pl.when(relayed(me + near, late))
            def _():
                slot = tile(relay, place)
                remote(slot, slot, parcel_send, relay_got.at[place], partner).wait_recv()
                target = tile(inbox, late)
                remote(slot, target, relay_send.at[place], got_parcel, me + near).start()

    @pl.when(is_owner)
    def _():
        mine = pl.ds(pl.multiple_of(me * 8, 8), 8)
        inbox[mine, :] = parcel[mine, :]
        arrived = inbox.at[pl.ds(0, (devices - 1) * 8), :]
        remote(arrived, arrived, parcel_send, got_parcel, partner).wait_recv()

    def data(k, t):
        return jnp.concatenate(
            [
                inbox[pl.ds(h * owners * 8 + k * 4 + t * 2 + e, owners, stride=8), :]
                for h in range(2)
                for e in range(local)
            ],
            axis=0,
        )

    fit_rows = fit_ref.shape[0]
    share = pair_box.shape[0]

    pair_send, pair_got, gather_send, gather_got = (sems.at[i] for i in range(1, 5))
    fit_got, row_send, row_got, residual_got, pass_send = (sems.at[i] for i in range(5, 10))

    def part(which):
        return folded_ref.at[pl.ds(pl.multiple_of(which * share, 8), share), :]

    pair = remote(part(1 - core), pair_box, pair_send, pair_got, partner)
    to_root = remote(sum_ref, gathered.at[me], gather_send, gather_got, root)

    @pl.when(is_owner)
    def _():
        total = gram(jnp.concatenate([data(k, t) for k in range(2) for t in range(halves)], axis=1))
        tiles = fold(total)
        folded_ref[...] = jnp.zeros_like(folded_ref)
        for i, value in enumerate(tiles):
            folded_ref[i * 8 : i * 8 + 8, :] = value
        pair.start()
        pair.wait_recv()
        mine = folded_ref[pl.ds(pl.multiple_of(core * share, 8), share), :] + pair_box[...]

        @pl.when(me == root)
        def _():
            gathered[me] = mine

        @pl.when(me != root)
        def _():
            sum_ref[...] = mine
            to_root.start()

    @pl.when(me == root)
    def _():
        known = systematics_ref.shape[0]
        templates = onsets_ref.shape[0]
        design_ref[...] = jnp.zeros_like(design_ref)
        design_ref[0:known, :] = systematics_ref[...]
        design_ref[...] = design_ref[...].T
        design = jnp.concatenate(
            [
                design_ref[pl.ds(h * owners * local + e, owners, stride=local), :]
                for h in range(2)
                for e in range(local)
            ],
            axis=0,
        )
        lane = iota((epochs, LANES), 1)
        place = iota((epochs, LANES), 0)
        group = place // owners
        epoch = lax.rem(place, owners) * local + (group // local) * owners * local
        epoch = epoch + lax.rem(group, local)
        onset = jnp.zeros((epochs, LANES), f32)
        for k in range(templates):
            onset = jnp.where(lane == known + k, onsets_ref[k].astype(f32), onset)
        delay = epoch.astype(f32) - onset
        timescale = (lane - known + 1).astype(f32) * epochs / (2.0 * templates)
        is_template = jnp.logical_and(lane >= known, lane < known + templates)
        timescale = jnp.where(is_template, timescale, 1.0)
        transient = jnp.where(delay >= 0.0, jnp.exp(-jnp.maximum(delay, 0.0) / timescale), 0.0)
        design = jnp.where(is_template, transient, design)
        base = dot_nt(design, design)
        diagonal = place == lane
        base = base + jnp.where(diagonal, cov_ridge, 0.0)

        slots = gathered.at[pl.ds(0, owners - 1)]
        remote(slots, slots, gather_send, gather_got, partner).wait_recv()
        total = [gathered[0], gathered[1]]
        for c in range(2, owners, 2):
            total = [t + gathered[c + s] for s, t in enumerate(total)]
        total = jnp.concatenate(total, axis=0)
        scatter = unfold([total[8 * i : 8 * i + 8, :] for i in range(LANES // 16 + 1)])
        gain = eliminate(base + scatter / pixels, design)
        fit_ref[...] = gain.T[0:fit_rows, :]

        for other in range(owners):
            if other != root:
                remote(fit_ref, fit_ref, fit_send.at[other], fit_got, other).start()

        projector = jnp.where(diagonal, 1.0, 0.0) - dot_nt(design, gain)
        product = jnp.dot(projector, scatter, precision=HIGHEST, preferred_element_type=f32)
        terms = product * projector
        for h in range(2):
            for e in range(local):
                at = (h * local + e) * owners
                design_ref[pl.ds(h * owners * local + e, owners, stride=local), :] = terms[
                    at : at + owners, :
                ]
        residual = jnp.sum(design_ref[...].T, axis=0, keepdims=True) / pixels
        residual_ref[...] = jnp.broadcast_to(residual, residual_ref.shape)
        for other in range(owners):
            if other != root:
                remote(
                    residual_ref, residual_ref, residual_send.at[other], residual_got, other
                ).start()

    def row(k):
        fit = fit_ref[...]
        return jnp.concatenate(
            [
                jnp.dot(fit, data(k, t), precision=HIGHEST, preferred_element_type=f32)
                for t in range(halves)
            ],
            axis=1,
        )

    fit_here = remote(fit_ref, fit_ref, fit_send.at[0], fit_got, partner)
    residual_here = remote(residual_ref, residual_ref, pass_send, residual_got, served)
    row_out = remote(row_ref, coefficients_ref, row_send, row_got, served)

    @pl.when(is_owner)
    def _():
        @pl.when(me != root)
        def _():
            fit_here.wait_recv()

        coefficients_ref[...] = row(0)
        row_ref[...] = row(1)
        row_out.start()

        @pl.when(me != root)
        def _():
            residual_here.wait_recv()

        residual_here.start()

        sent = parcel.at[pl.ds(0, (owners - 1) * 8), :]
        remote(sent, sent, parcel_send, got_parcel, partner).wait_send()

        @pl.when(me < near)
        def _():
            @pl.loop(0, near)
            def _(place):
                @pl.when(relayed(me + near, place + owners + near))
                def _():
                    slot = tile(relay, place)
                    remote(slot, slot, relay_send.at[place], got_parcel, partner).wait_send()

        pair.wait_send()

        @pl.when(me != root)
        def _():
            to_root.wait_send()

        row_out.wait_send()
        residual_here.wait_send()

    @pl.when(is_late)
    def _():
        remote(parcel, parcel, parcel_send, got_parcel, partner).wait_send()
        row_out.wait_recv()
        residual_here.wait_recv()

    @pl.when(me == root)
    def _():
        for other in range(owners):
            if other != root:
                remote(fit_ref, fit_ref, fit_send.at[other], fit_got, other).wait_send()
                remote(
                    residual_ref, residual_ref, residual_send.at[other], residual_got, other
                ).wait_send()


def finish(coefficients_ref, residual_ref, first_ref, second_ref):
    first_ref[...] = coefficients_ref[...].reshape(first_ref.shape)
    second_ref[...] = residual_ref[0]


def shards(
    devices, images, reference_image, kernels, kernel_index, tile_mask, systematics, onsets
):
    local, rows, width = images.shape
    side = kernels.shape[1]
    epochs = systematics.shape[0]
    columns = systematics.shape[1] + onsets.shape[0]
    owners = devices // 2
    near = owners // 2
    share = LANES // 8 // 4 * 8 + 8
    vmem = pl.BlockSpec(memory_space=pltpu.VMEM)
    smem = pl.BlockSpec(memory_space=pltpu.SMEM)
    dma = pltpu.SemaphoreType.DMA
    coefficients, residual = pl.pallas_call(
        functools.partial(body, devices),
        out_shape=(
            jax.ShapeDtypeStruct((columns, width), f32),
            jax.ShapeDtypeStruct((8, epochs), f32),
        ),
        in_specs=[smem, smem, vmem, vmem, vmem, vmem, vmem],
        out_specs=(vmem, vmem),
        scratch_shapes=[
            pltpu.VMEM((local, LANES, LANES), f32),
            pltpu.VMEM((local, side * rows, LANES), bf16),
            pltpu.VMEM((local, side * rows, width), f32),
            pltpu.VMEM((owners * 8, LANES), f32),
            pltpu.VMEM((devices * 8, LANES), f32),
            pltpu.VMEM((near * 8, LANES), f32),
            pltpu.VMEM((2 * share, epochs), f32),
            pltpu.VMEM((share, epochs), f32),
            pltpu.VMEM((share, epochs), f32),
            pltpu.VMEM((owners, share, epochs), f32),
            pltpu.VMEM((columns, epochs), f32),
            pltpu.VMEM((columns, width), f32),
            pltpu.VMEM((8, LANES), f32),
            pltpu.VMEM((epochs, LANES), f32),
            dma((10,)),
            dma,
            dma((near,)),
            dma((near,)),
            dma((owners,)),
            dma((owners,)),
        ],
        compiler_params=pltpu.CompilerParams(collective_id=0, has_side_effects=True),
    )(
        kernel_index,
        onsets,
        images,
        reference_image,
        jnp.transpose(kernels, (1, 0, 2)),
        jnp.transpose(tile_mask, (0, 2, 1)),
        systematics.T,
    )
    return pl.pallas_call(
        finish,
        out_shape=(
            jax.ShapeDtypeStruct((columns, 1, width), f32),
            jax.ShapeDtypeStruct((epochs,), f32),
        ),
        in_specs=[vmem, vmem],
        out_specs=(vmem, vmem),
    )(coefficients, residual)


def solution(mesh):
    in_specs = (
        P(("field", "ep"), None, None),
        P("field", None),
        P(),
        P(("field", "ep")),
        P(("field", "ep"), None, None),
        P("field", None),
        P("field"),
    )
    out_specs = (P(None, ("field", "ep"), None), P("field"))
    return jax.shard_map(
        functools.partial(shards, mesh.shape["ep"]),
        mesh=mesh,
        in_specs=in_specs,
        out_specs=out_specs,
        check_vma=False,
    )
```

```python
import functools

import jax
import jax.numpy as jnp
from jax import lax
from jax.experimental import pallas as pl
from jax.experimental.pallas import tpu as pltpu
from jax.sharding import PartitionSpec as P

f32, bf16, i32 = jnp.float32, jnp.bfloat16, jnp.int32
HIGHEST = lax.Precision.HIGHEST
cov_ridge = 0.5
LANES = 128


def split(x):
    high = x.astype(bf16).astype(f32)
    return high, x - high


def pieces(x):
    high, low = split(x)
    return high.astype(bf16), low.astype(bf16)


def iota(shape, axis):
    return lax.broadcasted_iota(i32, shape, axis)


def correlate(image, kernel, kpad, bands, shifted):
    side = kernel.shape[0]
    half = side // 2
    rows = image.shape[0]
    kpad[...] = jnp.zeros_like(kpad)
    kpad[0:side, 0:side] = kernel
    high, low = split(kpad[...].T)
    base = pltpu.roll(high, LANES - half, 1) + pltpu.roll(low, rows - half, 1)
    lane = iota((rows, LANES), 1)
    band = jnp.abs(lax.rem(lane, rows) - iota((rows, LANES), 0)) <= half
    for b in range(side):
        column = jnp.broadcast_to(base[b : b + 1, :], (rows, LANES))
        column = pltpu.roll(column, 0, 1, stride=1, stride_axis=0)
        bands[b * rows : (b + 1) * rows, :] = jnp.where(band, column, 0.0).astype(bf16)
    high, low = pieces(image)
    left = bands[...]
    shifted[...] = jnp.dot(
        jnp.concatenate([left, left], axis=1),
        jnp.concatenate([high, high, low, low], axis=0),
        preferred_element_type=f32,
    )
    total = [None, None]
    for b in range(side):
        s = b - half
        block = slice(b * rows, (b + 1) * rows)
        first, second = shifted[block, 0:LANES], shifted[block, LANES:]
        if s:
            x = pltpu.roll(first, (-s) % LANES, 1)
            y = pltpu.roll(second, (-s) % LANES, 1)
            if s > 0:
                inside = lane < LANES - s
                first, second = jnp.where(inside, x, y), jnp.where(inside, y, 0.0)
            else:
                inside = lane >= -s
                first, second = jnp.where(inside, x, 0.0), jnp.where(inside, y, x)
        total = [v if t is None else t + v for t, v in zip(total, (first, second))]
    return total


def eliminate(matrix, right):
    count = matrix.shape[0]
    width = 8
    row8 = iota((width, LANES), 0)
    for k in range(0, count, width):
        pivot = slice(k, k + width)
        columns = [
            jnp.broadcast_to(matrix[:, k + j : k + j + 1], (count, LANES)) for j in range(width)
        ]
        block = [c[pivot, :] for c in columns]
        a, x = matrix[pivot, :], right[pivot, :]
        for j in range(width):
            factor = block[j]
            inverse = 1.0 / factor[j : j + 1, :]

            def step(v):
                scaled = v[j : j + 1, :] * inverse
                return jnp.where(row8 == j, scaled, v - factor * scaled)

            a, x = step(a), step(x)
            for m in range(j + 1, width):
                block[m] = step(block[m])

        def update(value, rows):
            for j in range(width):
                value = value - columns[j] * rows[j : j + 1, :]
            above = [value[:k, :]] if k else []
            below = [value[k + width :, :]] if k + width < count else []
            return jnp.concatenate([*above, rows, *below], axis=0)

        if k + width < count:
            matrix = update(matrix, a)
        right = update(right, x)
    return right


NT = (((1,), (1,)), ((), ()))


def dot_nt(x, y):
    return lax.dot_general(x, y, NT, precision=HIGHEST, preferred_element_type=f32)


def gram(x):
    high, low = pieces(x)
    left = jnp.concatenate([high, high, low], axis=1)
    right = jnp.concatenate([high, low, high], axis=1)
    return lax.dot_general(left, right, NT, preferred_element_type=f32)


def fold(value):
    tiles = LANES // 8
    lane = iota((8, LANES), 1)
    block = [value[8 * i : 8 * i + 8, :] for i in range(tiles)]
    folded, last = [], jnp.zeros((8, LANES), f32)
    for i in range(tiles // 2):
        other = block[tiles - 1 - i]
        moved = pltpu.roll(other, 8 * i, 1) if i else other
        folded.append(jnp.where(lane >= 8 * i, block[i], moved))
        last = jnp.where(lane // 8 == tiles - 1 - i, other, last)
    return [*folded, last]


def unfold(folded):
    tiles = LANES // 8
    lane = iota((8, LANES), 1)
    above, blocks = [None] * tiles, [None] * tiles
    for i in range(tiles // 2):
        other = tiles - 1 - i
        moved = pltpu.roll(folded[i], LANES - 8 * i, 1) if i else folded[i]
        above[i] = jnp.where(lane >= 8 * i + 8, folded[i], 0.0)
        above[other] = jnp.where(lane >= 8 * other + 8, moved, 0.0)
        blocks[i] = jnp.where(lane // 8 == i, folded[i], 0.0)
        blocks[other] = jnp.where(lane // 8 == other, folded[-1], 0.0)
    above = jnp.concatenate(above, axis=0)
    return above + above.T + jnp.concatenate(blocks, axis=0)


def body(
    devices,
    index_ref,
    onsets_ref,
    images_hbm,
    reference_hbm,
    kernels_hbm,
    mask_hbm,
    systematics_hbm,
    coefficients_ref,
    residual_ref,
    images_ref,
    reference_ref,
    kernels_ref,
    mask_ref,
    systematics_ref,
    kpad,
    bands,
    shifted,
    parcel,
    inbox,
    relay_up,
    relay_down,
    folded_ref,
    pair_box,
    sum_ref,
    gathered,
    fit_ref,
    mask_pad,
    design_ref,
    load_sems,
    sems,
    fit_send,
    residual_send,
):
    local, rows, width = images_ref.shape
    epochs = systematics_ref.shape[1]
    halves = width // LANES
    root = 1
    pixels = float(rows * width)
    chips = devices // 2
    reach = chips // 4
    me = lax.axis_index("ep")
    core = lax.rem(me, 2)
    chip = me // 2
    partner = me + 1 - 2 * core

    def remote(source, target, send, receive, device):
        return pltpu.make_async_remote_copy(
            src_ref=source,
            dst_ref=target,
            send_sem=send,
            recv_sem=receive,
            device_id={"ep": device},
        )

    def at(offset, which):
        return lax.rem(chip + offset + chips, chips) * 2 + which

    close = [d * sign for d in range(reach, 0, -1) for sign in (1, -1)]

    barrier = pltpu.get_barrier_semaphore()
    for offset in close:
        for which in range(2):
            pl.semaphore_signal(barrier, inc=1, device_id={"ep": at(offset, which)})
    pl.semaphore_signal(barrier, inc=1, device_id={"ep": partner})

    loads = [
        pltpu.make_async_copy(source, target, load_sems.at[i])
        for i, (source, target) in enumerate(
            (
                (kernels_hbm, kernels_ref),
                (images_hbm, images_ref),
                (mask_hbm, mask_ref),
                (reference_hbm, reference_ref),
                (systematics_hbm, systematics_ref),
            )
        )
    ]
    for load in loads:
        load.start()
    for load in loads:
        load.wait()

    mask_pad[...] = jnp.zeros_like(mask_pad)
    for e in range(local):
        mask_pad[e * halves : (e + 1) * halves, 0:rows] = mask_ref[e].astype(f32)
    mask = mask_pad[...].T

    for e in range(local):
        conv = correlate(
            images_ref[e], kernels_ref[:, index_ref[e], :], kpad.at[e], bands.at[e], shifted.at[e]
        )
        for t in range(halves):
            lanes = slice(t * LANES, (t + 1) * LANES)
            line = e * halves + t
            good = jnp.broadcast_to(mask[0:rows, line : line + 1], (rows, LANES))
            parcel[:, line, :] = (reference_ref[:, lanes] - conv[t]) * good

    (
        parcel_send,
        got_piece,
        up_got,
        down_got,
        pass_send,
        pair_send,
        pair_got,
        gather_send,
        gather_got,
        fit_got,
        residual_got,
    ) = (sems.at[i] for i in range(11))

    pl.semaphore_wait(barrier, 4 * reach + 1)

    far = [(relay_up, up_got, reach, 1, chips // 2 - reach)]
    far.append((relay_down, down_got, -reach, -1, chips // 2 - reach - 1))
    for step in range(chips // 2 - reach, 0, -1):
        for box, got, first, sign, count in far:
            for which in range(2):
                if step <= count:
                    piece = parcel.at[at(first + sign * step, which)]
                    slot = box.at[2 * (step - 1) + which]
                    remote(piece, slot, parcel_send, got, at(first, core)).start()
    for offset in close:
        for which in range(2):
            other = at(offset, which)
            remote(parcel.at[other], inbox.at[me], parcel_send, got_piece, other).start()
    remote(parcel.at[partner], inbox.at[me], parcel_send, got_piece, partner).start()
    inbox[me] = parcel[me]
    for box, got, first, sign, count in far:
        remote(box, box, parcel_send, got, partner).wait_recv()
        for step in range(count, 0, -1):
            for which in range(2):
                target = inbox.at[at(-first, core)]
                piece = box.at[2 * (step - 1) + which]
                remote(piece, target, pass_send, got_piece, at(sign * step, which)).start()
    arrived = inbox.at[pl.ds(0, devices - 1)]
    remote(arrived, arrived, parcel_send, got_piece, partner).wait_recv()

    def data(t):
        return jnp.concatenate([inbox[:, e * halves + t, :] for e in range(local)], axis=0)

    fit_rows = fit_ref.shape[0]
    share = pair_box.shape[0]

    def part(which):
        return folded_ref.at[pl.ds(pl.multiple_of(which * share, 8), share), :]

    pair = remote(part(1 - core), pair_box, pair_send, pair_got, partner)
    to_root = remote(sum_ref, gathered.at[me], gather_send, gather_got, root)
    tiles = fold(gram(jnp.concatenate([data(t) for t in range(halves)], axis=1)))
    folded_ref[...] = jnp.zeros_like(folded_ref)
    for i, value in enumerate(tiles):
        folded_ref[i * 8 : i * 8 + 8, :] = value
    pair.start()
    pair.wait_recv()
    mine = folded_ref[pl.ds(pl.multiple_of(core * share, 8), share), :] + pair_box[...]

    @pl.when(me == root)
    def _():
        gathered[me] = mine

    @pl.when(me != root)
    def _():
        sum_ref[...] = mine
        to_root.start()

    @pl.when(me == root)
    def _():
        known = systematics_ref.shape[0]
        templates = onsets_ref.shape[0]
        design_ref[...] = jnp.zeros_like(design_ref)
        design_ref[0:known, :] = systematics_ref[...]
        design_ref[...] = design_ref[...].T
        design = jnp.concatenate(
            [design_ref[pl.ds(e, devices, stride=local), :] for e in range(local)], axis=0
        )
        lane = iota((epochs, LANES), 1)
        place = iota((epochs, LANES), 0)
        epoch = lax.rem(place, devices) * local + place // devices
        onset = jnp.zeros((epochs, LANES), f32)
        for k in range(templates):
            onset = jnp.where(lane == known + k, onsets_ref[k].astype(f32), onset)
        delay = epoch.astype(f32) - onset
        timescale = (lane - known + 1).astype(f32) * epochs / (2.0 * templates)
        is_template = jnp.logical_and(lane >= known, lane < known + templates)
        timescale = jnp.where(is_template, timescale, 1.0)
        transient = jnp.where(delay >= 0.0, jnp.exp(-jnp.maximum(delay, 0.0) / timescale), 0.0)
        design = jnp.where(is_template, transient, design)
        base = dot_nt(design, design)
        diagonal = place == lane
        base = base + jnp.where(diagonal, cov_ridge, 0.0)

        slots = gathered.at[pl.ds(0, devices - 1)]
        remote(slots, slots, gather_send, gather_got, partner).wait_recv()
        total = [gathered[0], gathered[1]]
        for c in range(2, devices, 2):
            total = [t + gathered[c + s] for s, t in enumerate(total)]
        total = jnp.concatenate(total, axis=0)
        scatter = unfold([total[8 * i : 8 * i + 8, :] for i in range(LANES // 16 + 1)])
        gain = eliminate(base + scatter / pixels, design)
        fit_ref[...] = gain.T[0:fit_rows, :]

        fits = []
        for offset in range(chips // 2 + 1):
            for other in ((offset, chips - offset) if 0 < offset < chips // 2 else (offset,)):
                fits += [2 * other + which for which in range(2) if 2 * other + which != root]
        for other in fits:
            remote(fit_ref, fit_ref, fit_send.at[other], fit_got, other).start()

        projector = jnp.where(diagonal, 1.0, 0.0) - dot_nt(design, gain)
        product = jnp.dot(projector, scatter, precision=HIGHEST, preferred_element_type=f32)
        terms = product * projector
        for e in range(local):
            design_ref[pl.ds(e, devices, stride=local), :] = terms[
                e * devices : (e + 1) * devices, :
            ]
        residual = jnp.sum(design_ref[...].T, axis=0, keepdims=True) / pixels
        residual_ref[...] = jnp.broadcast_to(residual, residual_ref.shape)
        for other in fits:
            remote(
                residual_ref, residual_ref, residual_send.at[other], residual_got, other
            ).start()

    fit_here = remote(fit_ref, fit_ref, parcel_send, fit_got, partner)
    residual_here = remote(residual_ref, residual_ref, parcel_send, residual_got, partner)

    @pl.when(me != root)
    def _():
        fit_here.wait_recv()

    for t in range(halves):
        coefficients_ref[:, t * LANES : (t + 1) * LANES] = jnp.dot(
            fit_ref[...], data(t), precision=HIGHEST, preferred_element_type=f32
        )

    sent = inbox.at[pl.ds(0, devices - 1)]
    remote(sent, sent, parcel_send, got_piece, partner).wait_send()
    for box, got, first, sign, count in far:
        remote(box, box, pass_send, got, partner).wait_send()
    pair.wait_send()

    @pl.when(me != root)
    def _():
        to_root.wait_send()
        residual_here.wait_recv()

    @pl.when(me == root)
    def _():
        for other in range(devices):
            if other != root:
                remote(fit_ref, fit_ref, fit_send.at[other], fit_got, other).wait_send()
                remote(
                    residual_ref, residual_ref, residual_send.at[other], residual_got, other
                ).wait_send()


def finish(coefficients_ref, residual_ref, first_ref, second_ref):
    first_ref[...] = coefficients_ref[...].reshape(first_ref.shape)
    second_ref[...] = residual_ref[0]


def shards(
    devices, images, reference_image, kernels, kernel_index, tile_mask, systematics, onsets
):
    local, rows, width = images.shape
    side = kernels.shape[1]
    epochs = systematics.shape[0]
    columns = systematics.shape[1] + onsets.shape[0]
    lines = local * width // LANES
    reach = devices // 8
    share = LANES // 8 // 4 * 8 + 8
    vmem = pl.BlockSpec(memory_space=pltpu.VMEM)
    smem = pl.BlockSpec(memory_space=pltpu.SMEM)
    anywhere = pl.BlockSpec(memory_space=pl.ANY)
    dma = pltpu.SemaphoreType.DMA
    inputs = (
        images,
        reference_image,
        jnp.transpose(kernels, (1, 0, 2)),
        jnp.transpose(tile_mask, (0, 2, 1)),
        systematics.T,
    )
    coefficients, residual = pl.pallas_call(
        functools.partial(body, devices),
        out_shape=(
            jax.ShapeDtypeStruct((columns, width), f32),
            jax.ShapeDtypeStruct((8, epochs), f32),
        ),
        in_specs=[smem, smem] + [anywhere] * len(inputs),
        out_specs=(vmem, vmem),
        scratch_shapes=[pltpu.VMEM(x.shape, x.dtype) for x in inputs]
        + [
            pltpu.VMEM((local, LANES, LANES), f32),
            pltpu.VMEM((local, side * rows, LANES), bf16),
            pltpu.VMEM((local, side * rows, width), f32),
            pltpu.VMEM((devices, lines, LANES), f32),
            pltpu.VMEM((devices, lines, LANES), f32),
            pltpu.VMEM((2 * reach, lines, LANES), f32),
            pltpu.VMEM((2 * reach - 2, lines, LANES), f32),
            pltpu.VMEM((2 * share, epochs), f32),
            pltpu.VMEM((share, epochs), f32),
            pltpu.VMEM((share, epochs), f32),
            pltpu.VMEM((devices, share, epochs), f32),
            pltpu.VMEM((columns, epochs), f32),
            pltpu.VMEM((8, LANES), f32),
            pltpu.VMEM((epochs, LANES), f32),
            dma((len(inputs),)),
            dma((11,)),
            dma((devices,)),
            dma((devices,)),
        ],
        compiler_params=pltpu.CompilerParams(collective_id=0, has_side_effects=True),
    )(kernel_index, onsets, *inputs)
    return pl.pallas_call(
        finish,
        out_shape=(
            jax.ShapeDtypeStruct((columns, 1, width), f32),
            jax.ShapeDtypeStruct((epochs,), f32),
        ),
        in_specs=[vmem, vmem],
        out_specs=(vmem, vmem),
    )(coefficients, residual)


def solution(mesh):
    in_specs = (
        P(("field", "ep"), None, None),
        P("field", None),
        P(),
        P(("field", "ep")),
        P(("field", "ep"), None, None),
        P("field", None),
        P("field"),
    )
    out_specs = (P(None, ("field", "ep"), None), P("field"))
    return jax.shard_map(
        functools.partial(shards, mesh.shape["ep"]),
        mesh=mesh,
        in_specs=in_specs,
        out_specs=out_specs,
        check_vma=False,
    )
```
